256 devices in a mesh: seq: 8 (over y, core), head: 32 (over x, z).
Axes of the slice: x: 4, y: 4, z: 8, core: 2. Of those that a mesh axis runs over, the one named last changes fastest.
Arguments:
- query: bfloat16 [32768, 4096], P(('seq', 'head')), may hold values from -6 to 6
- key_matrix: bfloat16 [32768, 2048], P(('seq', 'head')), may hold values from -6 to 6
- value_matrix: bfloat16 [32768, 2048], P(('seq', 'head')), may hold values from -6 to 6
- output_gradient: bfloat16 [32768, 4096], P(('seq', 'head')), may hold values from -6 to 6
- attn_out: bfloat16 [32768, 4096], P(('seq', 'head')), may hold values from -3 to 3
- doc_offsets: int32 [65], replicated, may hold values from 0 to 32768, as said below
- stats: float32 [32768, 32], P(('seq', 'head')), may hold values from -1 to 9
Outputs:
- grad_query: bfloat16 [32768, 4096], P(('seq', 'head'))
- key_gradient: bfloat16 [32768, 2048], P(('seq', 'head'))
- value_gradient: bfloat16 [32768, 2048], P(('seq', 'head'))
The draws below stay inside these ranges and needn't reach their ends.
Inputs may be any that keep to these rules, and one draw needn't show every extreme that they name: doc_offsets[0] is 0, doc_offsets[64] is 32768, the entries rise strictly; no document has more than 1023 tokens and one has exactly that many.
All inputs are finite; a program needn't handle non-finite values.
Results may differ from the reference program's by a relative error of at most 0.0063.
Values may be sent and summed in bfloat16 or wider, within the bound.
No kernel may reach another device: no remote copies, remote signals or barrier semaphores. Data moves between devices by JAX's collectives and lax.ppermute only.
A program may use at most 64 MiB of HBM per device.

```python
import jax
import jax.numpy as jnp
from jax import lax

HQ = 32
KEY_VALUE_HEADS = 16
HEAD_SIZE = 128
DOCHALF = 512
QBLK = 512
PACKED_TOKENS = 32768


def doc_bounds(key):
    frames = PACKED_TOKENS // DOCHALF
    base = jax.random.fold_in(key, 101)
    cut_key, pick_key = jax.random.split(base)
    index = jnp.arange(1, frames, dtype=jnp.int32)
    cuts = jax.random.randint(cut_key, (frames - 1,), 0, DOCHALF, dtype=jnp.int32)
    chosen = jax.random.randint(pick_key, (), 1, frames - 1, dtype=jnp.int32)
    cuts = jnp.where(index == chosen, 0, cuts)
    cuts = jnp.where(index == chosen + 1, DOCHALF - 1, cuts)
    inner = index * DOCHALF + cuts
    return jnp.concatenate([jnp.zeros((1,), jnp.int32), inner, jnp.full((1,), PACKED_TOKENS, jnp.int32)])


def draw_doc_offsets(key, part):
    return doc_bounds(key)


def draw_stats(key, part):
    bounds = doc_bounds(key)
    positions = jnp.arange(PACKED_TOKENS, dtype=jnp.int32)
    number = jnp.sum((bounds[1:-1][None, :] <= positions[:, None]).astype(jnp.int32), axis=1)
    starts = bounds[number]
    visible = (positions - starts + 1).astype(jnp.float32)
    noise_key = jax.random.fold_in(key, 202)
    spread = jax.random.uniform(noise_key, (PACKED_TOKENS, HQ), jnp.float32, -0.3, 0.3)
    return jnp.log(visible)[:, None] + 0.44 + spread


def level_of(own_key, shape, shards, least, largest):
    gain = 1.0
    for position, blocks in shards:
        draws = jax.random.uniform(jax.random.fold_in(jax.random.fold_in(own_key, 6), position), (blocks,), jnp.float32, least / len(shards), largest / len(shards))
        gain = gain * jnp.repeat(jnp.exp(draws), shape[position] // blocks).reshape((-1,) + (1,) * (len(shape) - 1 - position))
    return gain


def noise(key, extent, scale, most, cuts=(), kind=jnp.bfloat16):
    entries = scale * jax.random.normal(key, extent, jnp.float32)
    if cuts:
        entries = entries * level_of(key, extent, cuts, -0.22, 0.18)
    return jnp.clip(entries, -most, most).astype(kind)


def setup_inputs(seed: int = 0) -> dict:
    keys = jax.random.split(jax.random.key(seed), 8)
    return {
        "query": noise(keys[0], (PACKED_TOKENS, HQ * HEAD_SIZE), 1.0, 6.0, ((0, 256),)),
        "key_matrix": noise(keys[1], (PACKED_TOKENS, KEY_VALUE_HEADS * HEAD_SIZE), 1.0, 6.0, ((0, 256),)),
        "value_matrix": noise(keys[2], (PACKED_TOKENS, KEY_VALUE_HEADS * HEAD_SIZE), 1.0, 6.0, ((0, 256),)),
        "output_gradient": noise(keys[3], (PACKED_TOKENS, HQ * HEAD_SIZE), 1.0, 6.0, ((0, 256),)),
        "attn_out": noise(keys[4], (PACKED_TOKENS, HQ * HEAD_SIZE), 0.5, 3.0, ((0, 256),)),
        "doc_offsets": draw_doc_offsets(jax.random.fold_in(keys[7], 71), 0),
        "stats": draw_stats(jax.random.fold_in(keys[7], 71), 0),
    }


attn_scale = 144.0 ** -0.5


def tile_grads(query_rows, grad_rows, lse_rows, delta_rows, key_window, value_window, allowed):
    query_wide = query_rows.astype(jnp.float32)
    grad_wide = grad_rows.astype(jnp.float32)
    key_wide = key_window.astype(jnp.float32)
    value_wide = value_window.astype(jnp.float32)
    score = jnp.einsum("qgrd,kgd->grqk", query_wide, key_wide) * attn_scale
    norm_stat = jnp.transpose(lse_rows, (1, 2, 0))[..., None]
    prob = jnp.where(allowed[None, None], jnp.exp(score - norm_stat), 0.0)
    dprob = jnp.einsum("qgrd,kgd->grqk", grad_wide, value_wide)
    dscore = prob * (dprob - jnp.transpose(delta_rows, (1, 2, 0))[..., None])
    prob_low = prob.astype(jnp.bfloat16).astype(jnp.float32)
    dscore_low = dscore.astype(jnp.bfloat16).astype(jnp.float32)
    value_gradient = jnp.einsum("grqk,qgrd->kgd", prob_low, grad_wide)
    key_gradient = jnp.einsum("grqk,qgrd->kgd", dscore_low, query_wide) * attn_scale
    grad_query = jnp.einsum("grqk,kgd->qgrd", dscore_low, key_wide) * attn_scale
    return grad_query, key_gradient, value_gradient


def doc_numbers(positions, inner):
    return jnp.sum((inner[None, :] <= positions[:, None]).astype(jnp.int32), axis=1)


def reference(query, key_matrix, value_matrix, output_gradient, attn_out, doc_offsets, stats):
    lookback = 2 * DOCHALF
    width = lookback + QBLK
    inner = doc_offsets[1:-1]
    query_pos = jnp.arange(PACKED_TOKENS, dtype=jnp.int32)
    key_pos = jnp.arange(PACKED_TOKENS + lookback, dtype=jnp.int32) - lookback
    query_doc = doc_numbers(query_pos, inner)
    key_doc = doc_numbers(key_pos, inner)
    delta_correction = jnp.sum((output_gradient.astype(jnp.float32) * attn_out.astype(jnp.float32)).reshape(PACKED_TOKENS, HQ, HEAD_SIZE), axis=2)
    query_grouped = query.reshape(PACKED_TOKENS, KEY_VALUE_HEADS, 2, HEAD_SIZE)
    output_gradient_grouped = output_gradient.reshape(PACKED_TOKENS, KEY_VALUE_HEADS, 2, HEAD_SIZE)
    key_cube = key_matrix.reshape(PACKED_TOKENS, KEY_VALUE_HEADS, HEAD_SIZE)
    value_cube = value_matrix.reshape(PACKED_TOKENS, KEY_VALUE_HEADS, HEAD_SIZE)
    logsumexp_cube = stats.reshape(PACKED_TOKENS, KEY_VALUE_HEADS, 2)
    delta_correction_cube = delta_correction.reshape(PACKED_TOKENS, KEY_VALUE_HEADS, 2)
    padding = jnp.zeros((lookback, 1, HEAD_SIZE), jnp.bfloat16)

    def single_head_slice(head):
        query_head = query_grouped[:, head][:, None]
        grad_head = output_gradient_grouped[:, head][:, None]
        lse_head = logsumexp_cube[:, head][:, None]
        delta_head = delta_correction_cube[:, head][:, None]
        key_ext = jnp.concatenate([padding, key_cube[:, head][:, None]], 0)
        value_ext = jnp.concatenate([padding, value_cube[:, head][:, None]], 0)

        def block_step(block, carry):
            grad_q, grad_k, grad_v = carry
            start = (block * QBLK).astype(jnp.int32)
            query_rows = lax.dynamic_slice_in_dim(query_head, start, QBLK, 0)
            grad_rows = lax.dynamic_slice_in_dim(grad_head, start, QBLK, 0)
            lse_rows = lax.dynamic_slice_in_dim(lse_head, start, QBLK, 0)
            delta_rows = lax.dynamic_slice_in_dim(delta_head, start, QBLK, 0)
            key_window = lax.dynamic_slice_in_dim(key_ext, start, width, 0)
            value_window = lax.dynamic_slice_in_dim(value_ext, start, width, 0)
            rows_pos = lax.dynamic_slice_in_dim(query_pos, start, QBLK, 0)
            rows_doc = lax.dynamic_slice_in_dim(query_doc, start, QBLK, 0)
            cols_pos = lax.dynamic_slice_in_dim(key_pos, start, width, 0)
            cols_doc = lax.dynamic_slice_in_dim(key_doc, start, width, 0)
            allowed = (cols_doc[None, :] == rows_doc[:, None]) & (cols_pos[None, :] <= rows_pos[:, None]) & (cols_pos[None, :] >= 0)
            block_q, block_k, block_v = tile_grads(query_rows, grad_rows, lse_rows, delta_rows, key_window, value_window, allowed)
            grad_q = lax.dynamic_update_slice_in_dim(grad_q, block_q, start, 0)
            grad_k = lax.dynamic_update_slice_in_dim(grad_k, lax.dynamic_slice_in_dim(grad_k, start, width, 0) + block_k, start, 0)
            grad_v = lax.dynamic_update_slice_in_dim(grad_v, lax.dynamic_slice_in_dim(grad_v, start, width, 0) + block_v, start, 0)
            return grad_q, grad_k, grad_v

        init = (jnp.zeros((PACKED_TOKENS, 1, 2, HEAD_SIZE), jnp.float32), jnp.zeros((PACKED_TOKENS + lookback, 1, HEAD_SIZE), jnp.float32), jnp.zeros((PACKED_TOKENS + lookback, 1, HEAD_SIZE), jnp.float32))
        grad_q, grad_k, grad_v = lax.fori_loop(0, PACKED_TOKENS // QBLK, block_step, init)
        return grad_q[:, 0], grad_k[lookback:, 0], grad_v[lookback:, 0]

    every_query_row, every_key_row, every_value_row = lax.map(single_head_slice, jnp.arange(KEY_VALUE_HEADS, dtype=jnp.int32))
    grad_query = jnp.transpose(every_query_row, (1, 0, 2, 3)).reshape(PACKED_TOKENS, HQ * HEAD_SIZE).astype(jnp.bfloat16)
    key_gradient = jnp.transpose(every_key_row, (1, 0, 2)).reshape(PACKED_TOKENS, KEY_VALUE_HEADS * HEAD_SIZE).astype(jnp.bfloat16)
    value_gradient = jnp.transpose(every_value_row, (1, 0, 2)).reshape(PACKED_TOKENS, KEY_VALUE_HEADS * HEAD_SIZE).astype(jnp.bfloat16)
    return (grad_query, key_gradient, value_gradient)
```

```python
import functools

import jax
import jax.numpy as jnp
from jax import lax
from jax.experimental import pallas as pl
from jax.experimental.pallas import tpu as pltpu
from jax.sharding import PartitionSpec as P


HQ = 32
KV = 16
D = 128
TOK = 128
RING = 8
SPAN = RING * TOK
REPS = HQ // KV
QW = HQ // RING * D
KW = KV // RING * D
CHUNKS = KV // RING
MSG = 4 * TOK + 16
PAIR = 2 * TOK

attn_scale = 144.0 ** (-0.5)
LOG2E = 1.4426950408889634
F32 = jnp.float32
BF16 = jnp.bfloat16


ANY = pl.BlockSpec(memory_space=pl.ANY)
VM = pl.BlockSpec(memory_space=pltpu.VMEM)
SM = pl.BlockSpec(memory_space=pltpu.SMEM)


def dot_nt(a, b):
    return lax.dot_general(a, b, (((1,), (1,)), ((), ())), preferred_element_type=F32)


def dot_nn(a, b):
    return lax.dot_general(a, b, (((1,), (0,)), ((), ())), preferred_element_type=F32)


def in_vmem(shape, dtype):
    return pltpu.VMEM(shape, dtype)


def pack_keys_body(k, v, out, sem):
    copies = []
    for t in range(RING):
        for g in range(CHUNKS):
            col = t * KW + g * D
            for n, src in enumerate((k, v)):
                rows = pl.ds((2 * g + n) * TOK, TOK)
                c = pltpu.make_async_copy(src.at[:, pl.ds(col, D)], out.at[t, rows], sem.at[t, g, n])
                c.start()
                copies.append(c)
    for c in copies:
        c.wait()


def pack_keys(k, v):
    return pl.pallas_call(
        pack_keys_body,
        out_shape=in_vmem((RING, 2 * CHUNKS * TOK, D), BF16),
        in_specs=[ANY, ANY],
        out_specs=VM,
        scratch_shapes=[pltpu.SemaphoreType.DMA((RING, CHUNKS, 2))],
        name="packkv",
    )(k, v)


def pack_body(g, meta, stats_t, q, do, o, *rest):
    out = rest[:RING]
    o_s, sem = rest[RING:]
    z = meta[0]
    copies = []
    for d in range(RING):
        zt = lax.rem(z + d, RING)
        mine = []
        for r in range(REPS):
            col = pl.multiple_of(zt * QW + (g * REPS + r) * D, D)
            mine.append((q.at[:, pl.ds(col, D)], out[d].at[pl.ds(r * TOK, TOK)]))
            mine.append((do.at[:, pl.ds(col, D)], out[d].at[pl.ds((REPS + r) * TOK, TOK)]))
            mine.append((o.at[:, pl.ds(col, D)], o_s.at[d, r]))
        made = [pltpu.make_async_copy(a, b, sem.at[d, n]) for n, (a, b) in enumerate(mine)]
        for c in made:
            c.start()
        copies.append(made)
    ones = jnp.ones((16, D), BF16)
    row = lax.broadcasted_iota(jnp.int32, (16, TOK), 0)
    quarter = lax.rem(row, 4)
    for d in range(RING):
        zt = lax.rem(z + d, RING)
        for c in copies[d]:
            c.wait()
        stat = stats_t[zt]
        vals = [
            jnp.broadcast_to(stat[g * REPS + r : g * REPS + r + 1, :], (16, TOK))
            for r in range(REPS)
        ]
        for r in range(REPS):
            prod = out[d][pl.ds((REPS + r) * TOK, TOK), :].astype(F32) * o_s[d, r].astype(F32)
            high = prod.astype(BF16)
            low = (prod - high.astype(F32)).astype(BF16)
            vals.append(dot_nt(ones, high) + dot_nt(ones, low))
        x = vals[3]
        for n in range(3):
            x = jnp.where(quarter == n, vals[n], x)
        high = x.astype(BF16).astype(F32)
        rest1 = x - high
        mid = rest1.astype(BF16).astype(F32)
        low = (rest1 - mid).astype(BF16).astype(F32)
        x = jnp.where(row < 4, high, jnp.where(row < 8, mid, low))
        out[d][pl.ds(4 * TOK, 16), :] = x.astype(BF16)


def pack(g, meta, stats_t, q, do, o):
    return pl.pallas_call(
        functools.partial(pack_body, g),
        out_shape=[in_vmem((MSG, D), BF16)] * RING,
        in_specs=[SM, VM, ANY, ANY, ANY],
        out_specs=[VM] * RING,
        scratch_shapes=[
            pltpu.VMEM((RING, REPS, TOK, D), BF16),
            pltpu.SemaphoreType.DMA((RING, 3 * REPS)),
        ],
    )(meta, stats_t, q, do, o)


def attn_body(g, turned, meta, starts, keys, halo, *rest):
    msg = rest[:RING]
    n_out = RING if turned else 1
    out_q = rest[RING : RING + n_out]
    out_h, out_own = rest[RING + n_out : RING + n_out + 2]
    q_s, do_s, k_s, v_s, st_s, kt_s, dk_s, dv_s, dqt_s, dq_s, sem = rest[RING + n_out + 2 :]
    z = meta[0]
    copies = []
    for d in range(RING):
        zs = lax.rem(z - d + RING, RING)
        half = pl.ds((d % 2) * TOK, TOK)
        k_rows = pl.ds(2 * g * TOK, TOK)
        v_rows = pl.ds((2 * g + 1) * TOK, TOK)
        mine = [
            (msg[d].at[pl.ds(0, PAIR)], q_s.at[zs]),
            (msg[d].at[pl.ds(PAIR, PAIR)], do_s.at[zs]),
            (msg[d].at[pl.ds(2 * PAIR, 16)], st_s.at[zs]),
            (keys.at[d, k_rows], k_s.at[4 + d // 2, half]),
            (keys.at[d, v_rows], v_s.at[4 + d // 2, half]),
            (halo.at[d, k_rows], k_s.at[d // 2, half]),
            (halo.at[d, v_rows], v_s.at[d // 2, half]),
        ]
        for n, (a, b) in enumerate(mine):
            c = pltpu.make_async_copy(a, b, sem.at[d, n])
            c.start()
            copies.append(c)
    dk_s[...] = jnp.zeros(dk_s.shape, F32)
    dv_s[...] = jnp.zeros(dv_s.shape, F32)
    for c in copies:
        c.wait()

    def flip(jp, _):
        kt_s[jp] = k_s[jp].T
        return 0

    lax.fori_loop(meta[1], RING, flip, 0)
    key_at = lax.broadcasted_iota(jnp.int32, (PAIR, PAIR), 0)
    lane = lax.rem(lax.broadcasted_iota(jnp.int32, (1, PAIR), 1), TOK)

    def query_block(i, _):
        q = q_s[i]
        do = do_s[i]
        st = st_s[i].astype(F32)
        st = st[0:4] + st[4:8] + st[8:12]
        stat = jnp.concatenate([st[0:1], st[1:2]], axis=1) * LOG2E
        delta = jnp.concatenate([st[2:3], st[3:4]], axis=1)
        first = starts[pl.ds(i, 1), :]
        first = jnp.concatenate([first, first], axis=1)
        last = SPAN + i * TOK + lane
        dqt_s[...] = jnp.zeros(dqt_s.shape, F32)

        def key_block(jp, _):
            s = dot_nt(k_s[jp], q)
            p = jnp.exp2(s * (attn_scale * LOG2E) - stat)
            at = key_at + jp * PAIR
            p = jnp.where((at >= first) & (at <= last), p, 0.0)
            dp = dot_nt(v_s[jp], do)
            ds = (p * (dp - delta)).astype(BF16)
            dv_s[jp] += dot_nn(p.astype(BF16), do)
            dk_s[jp] += dot_nn(ds, q)
            dqt_s[...] += dot_nn(kt_s[jp], ds)
            return 0

        lax.fori_loop(meta[1 + i], 5 + i // 2, key_block, 0)
        dq_s[i] = (dqt_s[...] * attn_scale).T.astype(BF16)
        return 0

    lax.fori_loop(0, RING, query_block, 0)
    for d in range(RING):
        if turned:
            out_q[d][...] = dq_s[lax.rem(z + d, RING)]
        else:
            out_q[0][d] = dq_s[d]
        half = (d % 2) * TOK
        out_h[d, pl.ds(0, TOK), :] = (dk_s[d // 2, pl.ds(half, TOK), :] * attn_scale).astype(BF16)
        out_h[d, pl.ds(TOK, TOK), :] = dv_s[d // 2, pl.ds(half, TOK), :].astype(BF16)
        out_own[d, pl.ds(0, TOK), :] = dk_s[4 + d // 2, pl.ds(half, TOK), :] * attn_scale
        out_own[d, pl.ds(TOK, TOK), :] = dv_s[4 + d // 2, pl.ds(half, TOK), :]


def attn(g, turned, meta, starts, keys, halo, msgs):
    if turned:
        out_q = [in_vmem((PAIR, D), BF16)] * RING
    else:
        out_q = [in_vmem((RING, PAIR, D), BF16)]
    res = pl.pallas_call(
        functools.partial(attn_body, g, turned),
        out_shape=out_q + [in_vmem((RING, PAIR, D), BF16), in_vmem((RING, PAIR, D), F32)],
        in_specs=[SM, VM] + [ANY] * (RING + 2),
        out_specs=[VM] * (len(out_q) + 2),
        scratch_shapes=[
            pltpu.VMEM((RING, PAIR, D), BF16),
            pltpu.VMEM((RING, PAIR, D), BF16),
            pltpu.VMEM((RING, PAIR, D), BF16),
            pltpu.VMEM((RING, PAIR, D), BF16),
            pltpu.VMEM((RING, 16, TOK), BF16),
            pltpu.VMEM((RING, D, PAIR), BF16),
            pltpu.VMEM((RING, PAIR, D), F32),
            pltpu.VMEM((RING, PAIR, D), F32),
            pltpu.VMEM((D, PAIR), F32),
            pltpu.VMEM((RING, PAIR, D), BF16),
            pltpu.SemaphoreType.DMA((RING, 7)),
        ],
        cost_estimate=pl.CostEstimate(flops=3 * 10**9, bytes_accessed=4 * 10**6, transcendentals=0),
    )(meta, starts, keys, halo, *msgs)
    return res[:-2] if turned else res[0], res[-2], res[-1]


def finish_body(own, back, out):
    out[...] = (own[...] + back[...].astype(F32)).astype(BF16)


def finish(own, back):
    return pl.pallas_call(
        finish_body, out_shape=in_vmem((RING, PAIR, D), BF16), in_specs=[VM, VM], out_specs=VM
    )(own, back)


def unpack_q_body(meta, first, *rest):
    got = rest[:RING]
    dq = rest[RING]
    z = meta[0]
    for d in range(RING):
        zs = lax.rem(z - d + RING, RING)
        for r in range(REPS):
            dq[:, pl.ds(d * QW + r * D, D)] = first[d, pl.ds(r * TOK, TOK), :]
            col = pl.multiple_of(zs * QW + (REPS + r) * D, D)
            dq[:, pl.ds(col, D)] = got[d][pl.ds(r * TOK, TOK), :]


def unpack_q(meta, first, got):
    return pl.pallas_call(
        unpack_q_body,
        out_shape=jax.ShapeDtypeStruct((TOK, HQ * D), BF16),
        in_specs=[SM] + [VM] * (RING + 1),
        out_specs=VM,
        name="unpackq",
    )(meta, first, *got)


def unpack_kv_body(a, b, dk, dv):
    for d in range(RING):
        for g, src in enumerate((a, b)):
            cols = pl.ds(d * KW + g * D, D)
            dk[:, cols] = src[d, pl.ds(0, TOK), :]
            dv[:, cols] = src[d, pl.ds(TOK, TOK), :]


def unpack_kv(a, b):
    return pl.pallas_call(
        unpack_kv_body,
        out_shape=[jax.ShapeDtypeStruct((TOK, KV * D), BF16)] * 2,
        in_specs=[VM, VM],
        out_specs=[VM, VM],
        name="unpackkv",
    )(a, b)


def exchange(value):
    groups = lax.axis_size("head") // RING
    rows = [[g * RING + j for j in range(RING)] for g in range(groups)]
    return lax.all_to_all(value, "head", 0, 0, axis_index_groups=rows, tiled=True)


def ring_send(parts):
    groups = lax.axis_size("head") // RING
    got = [parts[0]] + [None] * (RING - 1)
    for d in (4, 1, 7, 2, 6, 3, 5):
        pairs = [
            (g * RING + j, g * RING + (j + d) % RING) for g in range(groups) for j in range(RING)
        ]
        got[d] = lax.ppermute(parts[d], "head", pairs)
    return got


def group_shift(value, step):
    axes = ("seq", "head")
    count = lax.axis_size("seq") * lax.axis_size("head")
    shift = RING * step
    pairs = [(s, s + shift) for s in range(count) if 0 <= s + shift < count]
    return lax.ppermute(value, axes, pairs)


def shards(query, key_matrix, value_matrix, output_gradient, attn_out, doc_offsets, stats):
    member = lax.axis_index("head")
    z = member % RING
    base = (lax.axis_index("seq") * lax.axis_size("head") + member - z) * TOK
    meta_z = z[None].astype(jnp.int32)
    keys = pack_keys(key_matrix, value_matrix)
    keys = exchange(keys)
    stats_t = stats.T.reshape(RING, HQ // RING, TOK)
    parts = pack(0, meta_z, stats_t, query, output_gradient, attn_out)
    got0 = ring_send(parts)
    parts = pack(1, meta_z, stats_t, query, output_gradient, attn_out)
    got1 = ring_send(parts)
    position = base + jnp.arange(SPAN, dtype=jnp.int32)
    inner = doc_offsets[1:-1]
    start = jnp.max(jnp.where(inner[None, :] <= position[:, None], inner[None, :], 0), axis=1)
    starts = (start - base + SPAN).reshape(RING, TOK)
    meta = jnp.concatenate([meta_z, starts[:, 0] // PAIR])
    halo = group_shift(keys, 1)
    dq0, back0, own0 = attn(0, False, meta, starts, keys, halo, got0)
    back0 = group_shift(back0, -1)
    dq0 = exchange(dq0)
    dq1, back1, own1 = attn(1, True, meta, starts, keys, halo, got1)
    back1 = group_shift(back1, -1)
    dkv0 = finish(own0, back0)
    dkv0 = exchange(dkv0)
    dq1 = ring_send(dq1)
    dkv1 = finish(own1, back1)
    dkv1 = exchange(dkv1)
    grad_query = unpack_q(meta_z, dq0, dq1)
    key_gradient, value_gradient = unpack_kv(dkv0, dkv1)
    return grad_query, key_gradient, value_gradient


def solution(mesh):
    placed = P(("seq", "head"), None)

    return jax.shard_map(
        shards,
        mesh=mesh,
        in_specs=(placed,) * 5 + (P(), placed),
        out_specs=(placed,) * 3,
        check_vma=False,
    )
```

```python
import functools

import jax
import jax.numpy as jnp
from jax import lax
from jax.experimental import pallas as pl
from jax.experimental.pallas import tpu as pltpu
from jax.sharding import PartitionSpec as P


HQ = 32
KV = 16
D = 128
TOK = 128
RING = 8
SPAN = RING * TOK
REPS = HQ // KV
QW = HQ // RING * D
KW = KV // RING * D
PAIR = 2 * TOK

attn_scale = 144.0 ** (-0.5)
LOG2E = 1.4426950408889634
F32 = jnp.float32
BF16 = jnp.bfloat16


ANY = pl.BlockSpec(memory_space=pl.ANY)
VM = pl.BlockSpec(memory_space=pltpu.VMEM)
SM = pl.BlockSpec(memory_space=pltpu.SMEM)


def dot_nt(a, b):
    return lax.dot_general(a, b, (((1,), (1,)), ((), ())), preferred_element_type=F32)


def dot_nn(a, b):
    return lax.dot_general(a, b, (((1,), (0,)), ((), ())), preferred_element_type=F32)


def leave(value):
    return pltpu.with_memory_space_constraint(value, pltpu.HBM)


def keep(value):
    return pltpu.with_memory_space_constraint(value, pltpu.VMEM)


def pack_keys_body(g, k, v, out, sem):
    copies = []
    for t in range(RING):
        for n, src in enumerate((k, v)):
            cols = pl.ds(t * KW + g * D, D)
            c = pltpu.make_async_copy(
                src.at[:, cols], out.at[t, pl.ds(n * TOK, TOK)], sem.at[t, n]
            )
            c.start()
            copies.append(c)
    for c in copies:
        c.wait()


def pack_keys(g, k, v):
    return pl.pallas_call(
        functools.partial(pack_keys_body, g),
        out_shape=pltpu.HBM((RING, PAIR, D), BF16),
        in_specs=[ANY, ANY],
        out_specs=VM,
        scratch_shapes=[pltpu.SemaphoreType.DMA((RING, 2))],
        compiler_params=pltpu.CompilerParams(vmem_limit_bytes=12 * 2**20),
    )(leave(k), leave(v))


def pack_body(g, ahead, meta, stats_t, q, do, o, *rest):
    n_in = 2 if ahead else 0
    keys = rest[:n_in]
    out = rest[n_in : n_in + RING]
    o_s, sem = rest[n_in + RING :]
    z = meta[0]
    copies = []
    for d in range(RING):
        zt = lax.rem(z + d, RING)
        mine = []
        for r in range(REPS):
            col = pl.multiple_of(zt * QW + (g * REPS + r) * D, D)
            mine.append((q.at[:, pl.ds(col, D)], out[d].at[pl.ds(r * TOK, TOK)]))
            mine.append((do.at[:, pl.ds(col, D)], out[d].at[pl.ds((REPS + r) * TOK, TOK)]))
            mine.append((o.at[:, pl.ds(col, D)], o_s.at[d, r]))
        col = pl.multiple_of(zt * KW + (g + 1) * D, D)
        for n, src in enumerate(keys):
            mine.append((src.at[:, pl.ds(col, D)], out[d].at[pl.ds((4 + n) * TOK, TOK)]))
        made = [pltpu.make_async_copy(a, b, sem.at[d, n]) for n, (a, b) in enumerate(mine)]
        for c in made:
            c.start()
        copies.append(made)
    ones = jnp.ones((16, D), BF16)
    row = lax.broadcasted_iota(jnp.int32, (16, TOK), 0)
    quarter = lax.rem(row, 4)
    for d in range(RING):
        zt = lax.rem(z + d, RING)
        for c in copies[d]:
            c.wait()
        stat = stats_t[zt]
        vals = [
            jnp.broadcast_to(stat[g * REPS + r : g * REPS + r + 1, :], (16, TOK))
            for r in range(REPS)
        ]
        for r in range(REPS):
            prod = out[d][pl.ds((REPS + r) * TOK, TOK), :].astype(F32) * o_s[d, r].astype(F32)
            high = prod.astype(BF16)
            low = (prod - high.astype(F32)).astype(BF16)
            vals.append(dot_nt(ones, high) + dot_nt(ones, low))
        x = vals[3]
        for n in range(3):
            x = jnp.where(quarter == n, vals[n], x)
        high = x.astype(BF16).astype(F32)
        rest1 = x - high
        mid = rest1.astype(BF16).astype(F32)
        low = (rest1 - mid).astype(BF16).astype(F32)
        x = jnp.where(row < 4, high, jnp.where(row < 8, mid, low))
        out[d][pl.ds((4 + n_in) * TOK, 16), :] = x.astype(BF16)


def pack(g, meta, stats_t, q, do, o, *keys):
    rows = (4 + len(keys)) * TOK + 16
    return pl.pallas_call(
        functools.partial(pack_body, g, len(keys) > 0),
        out_shape=[pltpu.HBM((rows, D), BF16)] * RING,
        in_specs=[SM, VM] + [ANY] * (3 + len(keys)),
        out_specs=[VM] * RING,
        scratch_shapes=[
            pltpu.VMEM((RING, REPS, TOK, D), BF16),
            pltpu.SemaphoreType.DMA((RING, 3 * REPS + len(keys))),
        ],
        compiler_params=pltpu.CompilerParams(vmem_limit_bytes=12 * 2**20),
    )(meta, leave(stats_t), *[leave(a) for a in (q, do, o) + keys])


def join_body(meta, *rest):
    msg = rest[:RING]
    out, sem = rest[RING:]
    copies = []
    for d in range(RING):
        zs = lax.rem(meta[0] - d + RING, RING)
        c = pltpu.make_async_copy(msg[d].at[pl.ds(4 * TOK, PAIR)], out.at[zs], sem.at[d])
        c.start()
        copies.append(c)
    for c in copies:
        c.wait()


def join(meta, msgs):
    return pl.pallas_call(
        join_body,
        out_shape=jax.ShapeDtypeStruct((RING, PAIR, D), BF16),
        in_specs=[SM] + [ANY] * RING,
        out_specs=VM,
        scratch_shapes=[pltpu.SemaphoreType.DMA((RING,))],
        compiler_params=pltpu.CompilerParams(vmem_limit_bytes=12 * 2**20),
        name="join",
    )(meta, *msgs)


def attn_body(meta, starts, keys, halo, *rest):
    msg = rest[:RING]
    out_q, out_h, out_own = rest[RING : RING + 3]
    q_s, do_s, k_s, v_s, st_s, kt_s, dk_s, dv_s, dqt_s = rest[RING + 3 :]
    z = meta[0]
    tail = msg[0].shape[0] - 16
    for d in range(RING):
        zs = lax.rem(z - d + RING, RING)
        q_s[zs] = msg[d][pl.ds(0, PAIR), :]
        do_s[zs] = msg[d][pl.ds(PAIR, PAIR), :]
        st_s[zs] = msg[d][pl.ds(tail, 16), :]
    dk_s[...] = jnp.zeros(dk_s.shape, F32)
    dv_s[...] = jnp.zeros(dv_s.shape, F32)

    def gather(jp, src, at):
        for n in range(2):
            half = pl.ds(n * TOK, TOK)
            k = src[2 * at + n, pl.ds(0, TOK), :]
            k_s[jp, half, :] = k
            v_s[jp, half, :] = src[2 * at + n, pl.ds(TOK, TOK), :]
            kt_s[jp, :, half] = k.T
        return 0

    lax.fori_loop(meta[1], RING // 2, lambda jp, _: gather(jp, halo, jp), 0)
    for jp in range(RING // 2):
        gather(RING // 2 + jp, keys, jp)
    key_at = lax.broadcasted_iota(jnp.int32, (PAIR, 2 * PAIR), 0)
    lane = lax.rem(lax.broadcasted_iota(jnp.int32, (1, 2 * PAIR), 1), TOK)
    block = lax.broadcasted_iota(jnp.int32, (1, 2 * PAIR), 1) // PAIR
    own_at = lane + block * TOK

    def query_block(m, _):
        q = q_s[pl.ds(2 * m, 2)].reshape(2 * PAIR, D)
        do = do_s[pl.ds(2 * m, 2)].reshape(2 * PAIR, D)
        stat, delta, first = [], [], []
        for n in range(2):
            st = st_s[2 * m + n].astype(F32)
            st = st[0:4] + st[4:8] + st[8:12]
            stat += [st[0:1], st[1:2]]
            delta += [st[2:3], st[3:4]]
            row = starts[pl.ds(2 * m + n, 1), :]
            first += [row, row]
        stat = jnp.concatenate(stat, axis=1) * LOG2E
        delta = jnp.concatenate(delta, axis=1)
        first = jnp.concatenate(first, axis=1)

        def tile(jp, diagonal):
            s = dot_nt(k_s[jp], q)
            p = jnp.exp2(s * (attn_scale * LOG2E) - stat)
            p = jnp.where(key_at >= first - jp * PAIR, p, 0.0)
            if diagonal:
                p = jnp.where(key_at <= own_at, p, 0.0)
            dp = dot_nt(v_s[jp], do)
            ds = (p * (dp - delta)).astype(BF16)
            dv_s[jp] += dot_nn(p.astype(BF16), do)
            dk_s[jp] += dot_nn(ds, q)
            return dot_nn(kt_s[jp], ds)

        dqt_s[...] = tile(RING // 2 + m, True)

        def key_block(jp, _):
            dqt_s[...] += tile(jp, False)
            return 0

        lax.fori_loop(meta[1 + 2 * m], RING // 2 + m, key_block, 0)
        dq = (dqt_s[...] * attn_scale).T.astype(BF16)
        out_q[2 * m] = dq[:PAIR]
        out_q[2 * m + 1] = dq[PAIR:]
        return 0

    lax.fori_loop(0, RING // 2, query_block, 0)
    for d in range(RING):
        half = pl.ds((d % 2) * TOK, TOK)
        out_h[d, pl.ds(0, TOK), :] = (dk_s[d // 2, half, :] * attn_scale).astype(BF16)
        out_h[d, pl.ds(TOK, TOK), :] = dv_s[d // 2, half, :].astype(BF16)
        out_own[d, pl.ds(0, TOK), :] = dk_s[4 + d // 2, half, :] * attn_scale
        out_own[d, pl.ds(TOK, TOK), :] = dv_s[4 + d // 2, half, :]


def attn(g, meta, starts, keys, halo, msgs, hold):
    return pl.pallas_call(
        attn_body,
        out_shape=[
            (pltpu.HBM if g == 0 else pltpu.VMEM)((RING, PAIR, D), BF16),
            pltpu.VMEM((RING, PAIR, D), BF16),
            pltpu.VMEM((RING, PAIR, D), F32),
        ],
        in_specs=[SM, VM] + [VM] * (RING + 2),
        out_specs=[VM] * 3,
        scratch_shapes=[
            pltpu.VMEM((RING, PAIR, D), BF16),
            pltpu.VMEM((RING, PAIR, D), BF16),
            pltpu.VMEM((RING, PAIR, D), BF16),
            pltpu.VMEM((RING, PAIR, D), BF16),
            pltpu.VMEM((RING, 16, TOK), BF16),
            pltpu.VMEM((RING, D, PAIR), BF16),
            pltpu.VMEM((RING, PAIR, D), F32),
            pltpu.VMEM((RING, PAIR, D), F32),
            pltpu.VMEM((D, 2 * PAIR), F32),
        ],
        cost_estimate=pl.CostEstimate(flops=3 * 10**9, bytes_accessed=4 * 10**6, transcendentals=0),
        compiler_params=pltpu.CompilerParams(vmem_limit_bytes=16 * 2**20),
    )(meta, starts, hold(keys), hold(halo), msgs[0], *[hold(m) for m in msgs[1:]])


def merge_body(meta, dq, own, back, *out):
    for d in range(RING):
        zt = lax.rem(meta[0] + d, RING)
        out[d][pl.ds(0, PAIR), :] = dq[zt]
        out[d][pl.ds(PAIR, PAIR), :] = (own[zt] + back[zt].astype(F32)).astype(BF16)


def merge(meta, dq, own, back):
    return pl.pallas_call(
        merge_body,
        out_shape=[pltpu.HBM((2 * PAIR, D), BF16)] * RING,
        in_specs=[SM, VM, VM, VM],
        out_specs=[VM] * RING,
        compiler_params=pltpu.CompilerParams(vmem_limit_bytes=12 * 2**20),
        name="merge",
    )(meta, keep(dq), keep(own), keep(back))


def finish_body(own, back, out):
    out[...] = (own[...] + back[...].astype(F32)).astype(BF16)


def finish(own, back):
    return pl.pallas_call(
        finish_body,
        out_shape=pltpu.HBM((RING, PAIR, D), BF16),
        in_specs=[VM, VM],
        out_specs=VM,
        compiler_params=pltpu.CompilerParams(vmem_limit_bytes=12 * 2**20),
        name="finish",
    )(keep(own), keep(back))


def unpack_q_body(meta, first, *rest):
    got = rest[:RING]
    dq, dkv = rest[RING:]
    for d in range(RING):
        zs = lax.rem(meta[0] - d + RING, RING)
        dkv[zs] = got[d][pl.ds(PAIR, PAIR), :]
        for r in range(REPS):
            dq[:, pl.ds(d * QW + r * D, D)] = first[d, pl.ds(r * TOK, TOK), :]
            col = pl.multiple_of(zs * QW + (REPS + r) * D, D)
            dq[:, pl.ds(col, D)] = got[d][pl.ds(r * TOK, TOK), :]


def unpack_q(meta, first, got):
    return pl.pallas_call(
        unpack_q_body,
        out_shape=[
            jax.ShapeDtypeStruct((TOK, HQ * D), BF16),
            pltpu.VMEM((RING, PAIR, D), BF16),
        ],
        in_specs=[SM] + [VM] * (RING + 1),
        out_specs=[VM, VM],
        compiler_params=pltpu.CompilerParams(vmem_limit_bytes=12 * 2**20),
        name="unpackq",
    )(meta, keep(first), got[0], *[keep(m) for m in got[1:]])


def unpack_kv_body(a, b, dk, dv):
    for d in range(RING):
        for g, src in enumerate((a, b)):
            cols = pl.ds(d * KW + g * D, D)
            dk[:, cols] = src[d, pl.ds(0, TOK), :]
            dv[:, cols] = src[d, pl.ds(TOK, TOK), :]


def unpack_kv(a, b):
    return pl.pallas_call(
        unpack_kv_body,
        out_shape=[jax.ShapeDtypeStruct((TOK, KV * D), BF16)] * 2,
        in_specs=[VM, VM],
        out_specs=[VM, VM],
        compiler_params=pltpu.CompilerParams(vmem_limit_bytes=12 * 2**20),
        name="unpackkv",
    )(keep(a), keep(b))


def exchange(value):
    groups = lax.axis_size("head") // RING
    rows = [[g * RING + j for j in range(RING)] for g in range(groups)]
    return lax.all_to_all(value, "head", 0, 0, axis_index_groups=rows, tiled=True)


DISTANCES = (1, 7, 2, 6, 3, 5, 4)


def ring_send(parts):
    groups = lax.axis_size("head") // RING
    got = [parts[0]] + [None] * (RING - 1)
    for d in DISTANCES:
        pairs = [
            (g * RING + j, g * RING + (j + d) % RING) for g in range(groups) for j in range(RING)
        ]
        got[d] = lax.ppermute(parts[d], "head", pairs)
    return got


def group_shift(value, step):
    axes = ("seq", "head")
    count = lax.axis_size("seq") * lax.axis_size("head")
    shift = RING * step
    pairs = [(s, s + shift) for s in range(count) if 0 <= s + shift < count]
    return lax.ppermute(value, axes, pairs)


def shards(query, key_matrix, value_matrix, output_gradient, attn_out, doc_offsets, stats):
    member = lax.axis_index("head")
    z = member % RING
    base = (lax.axis_index("seq") * lax.axis_size("head") + member - z) * TOK
    meta_z = z[None].astype(jnp.int32)
    stats_t = stats.T.reshape(RING, HQ // RING, TOK)
    rows = (query, output_gradient, attn_out)
    keys0 = pack_keys(0, key_matrix, value_matrix)
    keys0 = exchange(keys0)
    parts = pack(0, meta_z, stats_t, *rows, key_matrix, value_matrix)
    got0 = ring_send(parts)
    halo0 = group_shift(keys0, 1)
    parts = pack(1, meta_z, stats_t, *rows)
    got1 = ring_send(parts)
    keys1 = join(meta_z, got0)
    halo1 = group_shift(keys1, 1)
    position = base + jnp.arange(SPAN, dtype=jnp.int32)
    inner = doc_offsets[1:-1]
    start = jnp.max(jnp.where(inner[None, :] <= position[:, None], inner[None, :], 0), axis=1)
    starts = (start - base + SPAN).reshape(RING, TOK)
    meta = jnp.concatenate([meta_z, starts[:, 0] // PAIR])
    dq0, back0, own0 = attn(0, meta, starts, keys0, halo0, got0, keep)
    back0 = group_shift(back0, -1)
    dq0 = exchange(dq0)
    dq1, back1, own1 = attn(1, meta, starts, keys1, halo1, got1, lambda m: m)
    back1 = group_shift(back1, -1)
    parts = merge(meta_z, dq1, own0, back0)
    mixed = ring_send(parts)
    dkv1 = finish(own1, back1)
    dkv1 = exchange(dkv1)
    grad_query, dkv0 = unpack_q(meta_z, dq0, mixed)
    key_gradient, value_gradient = unpack_kv(dkv0, dkv1)
    return grad_query, key_gradient, value_gradient


def solution(mesh):
    placed = P(("seq", "head"), None)

    return jax.shard_map(
        shards,
        mesh=mesh,
        in_specs=(placed,) * 5 + (P(), placed),
        out_specs=(placed,) * 3,
        check_vma=False,
    )
```

```python
import functools

import jax
import jax.numpy as jnp
from jax import lax
from jax.experimental import pallas as pl
from jax.experimental.pallas import tpu as pltpu
from jax.sharding import PartitionSpec as P


HQ = 32
KV = 16
D = 128
TOK = 128
RING = 8
SPAN = RING * TOK
REPS = HQ // KV
QW = HQ // RING * D
KW = KV // RING * D
PAIR = 2 * TOK

attn_scale = 144.0 ** (-0.5)
LOG2E = 1.4426950408889634
F32 = jnp.float32
BF16 = jnp.bfloat16


ANY = pl.BlockSpec(memory_space=pl.ANY)
VM = pl.BlockSpec(memory_space=pltpu.VMEM)
SM = pl.BlockSpec(memory_space=pltpu.SMEM)


def dot_nt(a, b):
    return lax.dot_general(a, b, (((1,), (1,)), ((), ())), preferred_element_type=F32)


def dot_nn(a, b):
    return lax.dot_general(a, b, (((1,), (0,)), ((), ())), preferred_element_type=F32)


def leave(value):
    return pltpu.with_memory_space_constraint(value, pltpu.HBM)


def keep(value):
    return pltpu.with_memory_space_constraint(value, pltpu.VMEM)


def pack_keys_body(g, k, v, out, sem):
    copies = []
    for t in range(RING):
        for n, src in enumerate((k, v)):
            cols = pl.ds(t * KW + g * D, D)
            c = pltpu.make_async_copy(
                src.at[:, cols], out.at[t, pl.ds(n * TOK, TOK)], sem.at[t, n]
            )
            c.start()
            copies.append(c)
    for c in copies:
        c.wait()


def pack_keys(g, k, v):
    return pl.pallas_call(
        functools.partial(pack_keys_body, g),
        out_shape=pltpu.HBM((RING, PAIR, D), BF16),
        in_specs=[ANY, ANY],
        out_specs=VM,
        scratch_shapes=[pltpu.SemaphoreType.DMA((RING, 2))],
        compiler_params=pltpu.CompilerParams(vmem_limit_bytes=12 * 2**20),
    )(leave(k), leave(v))


def pack_body(g, dists, ahead, meta, stats_t, q, do, o, *rest):
    n_in = 2 if ahead else 0
    keys = rest[:n_in]
    out = rest[n_in : n_in + len(dists)]
    o_s, sem = rest[n_in + len(dists) :]
    z = meta[0]
    copies = []
    for d, dist in enumerate(dists):
        zt = lax.rem(z + dist, RING)
        mine = []
        for r in range(REPS):
            col = pl.multiple_of(zt * QW + (g * REPS + r) * D, D)
            mine.append((q.at[:, pl.ds(col, D)], out[d].at[pl.ds(r * TOK, TOK)]))
            mine.append((do.at[:, pl.ds(col, D)], out[d].at[pl.ds((REPS + r) * TOK, TOK)]))
            mine.append((o.at[:, pl.ds(col, D)], o_s.at[d, r]))
        col = pl.multiple_of(zt * KW + (g + 1) * D, D)
        for n, src in enumerate(keys):
            mine.append((src.at[:, pl.ds(col, D)], out[d].at[pl.ds((4 + n) * TOK, TOK)]))
        made = [pltpu.make_async_copy(a, b, sem.at[d, n]) for n, (a, b) in enumerate(mine)]
        for c in made:
            c.start()
        copies.append(made)
    ones = jnp.ones((16, D), BF16)
    row = lax.broadcasted_iota(jnp.int32, (16, TOK), 0)
    quarter = lax.rem(row, 4)
    for d, dist in enumerate(dists):
        zt = lax.rem(z + dist, RING)
        for c in copies[d]:
            c.wait()
        stat = stats_t[zt]
        vals = [
            jnp.broadcast_to(stat[g * REPS + r : g * REPS + r + 1, :], (16, TOK))
            for r in range(REPS)
        ]
        for r in range(REPS):
            prod = out[d][pl.ds((REPS + r) * TOK, TOK), :].astype(F32) * o_s[d, r].astype(F32)
            high = prod.astype(BF16)
            low = (prod - high.astype(F32)).astype(BF16)
            vals.append(dot_nt(ones, high) + dot_nt(ones, low))
        x = vals[3]
        for n in range(3):
            x = jnp.where(quarter == n, vals[n], x)
        high = x.astype(BF16).astype(F32)
        rest1 = x - high
        mid = rest1.astype(BF16).astype(F32)
        low = (rest1 - mid).astype(BF16).astype(F32)
        x = jnp.where(row < 4, high, jnp.where(row < 8, mid, low))
        out[d][pl.ds((4 + n_in) * TOK, 16), :] = x.astype(BF16)


def pack(g, dists, meta, stats_t, q, do, o, *keys):
    rows = (4 + len(keys)) * TOK + 16
    made = pl.pallas_call(
        functools.partial(pack_body, g, dists, len(keys) > 0),
        out_shape=[pltpu.HBM((rows, D), BF16)] * len(dists),
        in_specs=[SM, VM] + [ANY] * (3 + len(keys)),
        out_specs=[VM] * len(dists),
        scratch_shapes=[
            pltpu.VMEM((len(dists), REPS, TOK, D), BF16),
            pltpu.SemaphoreType.DMA((len(dists), 3 * REPS + len(keys))),
        ],
        compiler_params=pltpu.CompilerParams(vmem_limit_bytes=12 * 2**20),
    )(meta, leave(stats_t), *[leave(a) for a in (q, do, o) + keys])
    return dict(zip(dists, made))


def join_body(meta, *rest):
    msg = rest[:RING]
    out, sem = rest[RING:]
    copies = []
    for d in range(RING):
        zs = lax.rem(meta[0] - d + RING, RING)
        c = pltpu.make_async_copy(msg[d].at[pl.ds(4 * TOK, PAIR)], out.at[zs], sem.at[d])
        c.start()
        copies.append(c)
    for c in copies:
        c.wait()


def join(meta, msgs):
    return pl.pallas_call(
        join_body,
        out_shape=jax.ShapeDtypeStruct((RING, PAIR, D), BF16),
        in_specs=[SM] + [ANY] * RING,
        out_specs=VM,
        scratch_shapes=[pltpu.SemaphoreType.DMA((RING,))],
        compiler_params=pltpu.CompilerParams(vmem_limit_bytes=12 * 2**20),
        name="join",
    )(meta, *msgs)


def attn_body(meta, starts, keys, halo, *rest):
    msg = rest[:RING]
    out_q, out_h, out_own = rest[RING : RING + 3]
    q_s, do_s, k_s, v_s, st_s, kt_s, dk_s, dv_s, dqt_s = rest[RING + 3 :]
    z = meta[0]
    tail = msg[0].shape[0] - 16
    for d in range(RING):
        zs = lax.rem(z - d + RING, RING)
        q_s[zs] = msg[d][pl.ds(0, PAIR), :]
        do_s[zs] = msg[d][pl.ds(PAIR, PAIR), :]
        st_s[zs] = msg[d][pl.ds(tail, 16), :]
    dk_s[...] = jnp.zeros(dk_s.shape, F32)
    dv_s[...] = jnp.zeros(dv_s.shape, F32)

    def gather(jp, src, at):
        for n in range(2):
            half = pl.ds(n * TOK, TOK)
            k = src[2 * at + n, pl.ds(0, TOK), :]
            k_s[jp, half, :] = k
            v_s[jp, half, :] = src[2 * at + n, pl.ds(TOK, TOK), :]
            kt_s[jp, :, half] = k.T
        return 0

    lax.fori_loop(meta[1], RING // 2, lambda jp, _: gather(jp, halo, jp), 0)
    for jp in range(RING // 2):
        gather(RING // 2 + jp, keys, jp)
    key_at = lax.broadcasted_iota(jnp.int32, (PAIR, 2 * PAIR), 0)
    lane = lax.rem(lax.broadcasted_iota(jnp.int32, (1, 2 * PAIR), 1), TOK)
    block = lax.broadcasted_iota(jnp.int32, (1, 2 * PAIR), 1) // PAIR
    own_at = lane + block * TOK

    def query_block(m, _):
        q = q_s[pl.ds(2 * m, 2)].reshape(2 * PAIR, D)
        do = do_s[pl.ds(2 * m, 2)].reshape(2 * PAIR, D)
        stat, delta, first = [], [], []
        for n in range(2):
            st = st_s[2 * m + n].astype(F32)
            st = st[0:4] + st[4:8] + st[8:12]
            stat += [st[0:1], st[1:2]]
            delta += [st[2:3], st[3:4]]
            row = starts[pl.ds(2 * m + n, 1), :]
            first += [row, row]
        stat = jnp.concatenate(stat, axis=1) * LOG2E
        delta = jnp.concatenate(delta, axis=1)
        first = jnp.concatenate(first, axis=1)

        def tile(jp, diagonal):
            s = dot_nt(k_s[jp], q)
            p = jnp.exp2(s * (attn_scale * LOG2E) - stat)
            p = jnp.where(key_at >= first - jp * PAIR, p, 0.0)
            if diagonal:
                p = jnp.where(key_at <= own_at, p, 0.0)
            dp = dot_nt(v_s[jp], do)
            ds = (p * (dp - delta)).astype(BF16)
            dv_s[jp] += dot_nn(p.astype(BF16), do)
            dk_s[jp] += dot_nn(ds, q)
            return dot_nn(kt_s[jp], ds)

        dqt_s[...] = tile(RING // 2 + m, True)

        def key_block(jp, _):
            dqt_s[...] += tile(jp, False)
            return 0

        lax.fori_loop(meta[1 + 2 * m], RING // 2 + m, key_block, 0)
        dq = (dqt_s[...] * attn_scale).T.astype(BF16)
        out_q[2 * m] = dq[:PAIR]
        out_q[2 * m + 1] = dq[PAIR:]
        return 0

    lax.fori_loop(0, RING // 2, query_block, 0)
    for d in range(RING):
        half = pl.ds((d % 2) * TOK, TOK)
        out_h[d, pl.ds(0, TOK), :] = (dk_s[d // 2, half, :] * attn_scale).astype(BF16)
        out_h[d, pl.ds(TOK, TOK), :] = dv_s[d // 2, half, :].astype(BF16)
        out_own[d, pl.ds(0, TOK), :] = dk_s[4 + d // 2, half, :] * attn_scale
        out_own[d, pl.ds(TOK, TOK), :] = dv_s[4 + d // 2, half, :]


def attn(g, meta, starts, keys, halo, msgs, hold):
    return pl.pallas_call(
        attn_body,
        out_shape=[
            (pltpu.HBM if g == 0 else pltpu.VMEM)((RING, PAIR, D), BF16),
            pltpu.VMEM((RING, PAIR, D), BF16),
            pltpu.VMEM((RING, PAIR, D), F32),
        ],
        in_specs=[SM, VM] + [VM] * (RING + 2),
        out_specs=[VM] * 3,
        scratch_shapes=[
            pltpu.VMEM((RING, PAIR, D), BF16),
            pltpu.VMEM((RING, PAIR, D), BF16),
            pltpu.VMEM((RING, PAIR, D), BF16),
            pltpu.VMEM((RING, PAIR, D), BF16),
            pltpu.VMEM((RING, 16, TOK), BF16),
            pltpu.VMEM((RING, D, PAIR), BF16),
            pltpu.VMEM((RING, PAIR, D), F32),
            pltpu.VMEM((RING, PAIR, D), F32),
            pltpu.VMEM((D, 2 * PAIR), F32),
        ],
        cost_estimate=pl.CostEstimate(flops=3 * 10**9, bytes_accessed=4 * 10**6, transcendentals=0),
        compiler_params=pltpu.CompilerParams(vmem_limit_bytes=16 * 2**20),
    )(meta, starts, hold(keys), hold(halo), msgs[0], *[hold(m) for m in msgs[1:]])


def merge_body(meta, dq, own, back, *out):
    for d in range(RING):
        zt = lax.rem(meta[0] + d, RING)
        out[d][pl.ds(0, PAIR), :] = dq[zt]
        out[d][pl.ds(PAIR, PAIR), :] = (own[zt] + back[zt].astype(F32)).astype(BF16)


def merge(meta, dq, own, back):
    return pl.pallas_call(
        merge_body,
        out_shape=[pltpu.HBM((2 * PAIR, D), BF16)] * RING,
        in_specs=[SM, VM, VM, VM],
        out_specs=[VM] * RING,
        compiler_params=pltpu.CompilerParams(vmem_limit_bytes=12 * 2**20),
        name="merge",
    )(meta, keep(dq), keep(own), keep(back))


def finish_body(own, back, out):
    out[...] = (own[...] + back[...].astype(F32)).astype(BF16)


def finish(own, back):
    return pl.pallas_call(
        finish_body,
        out_shape=pltpu.HBM((RING, PAIR, D), BF16),
        in_specs=[VM, VM],
        out_specs=VM,
        compiler_params=pltpu.CompilerParams(vmem_limit_bytes=12 * 2**20),
        name="finish",
    )(keep(own), keep(back))


def unpack_q_body(meta, first, *rest):
    got = rest[:RING]
    dq, dkv = rest[RING:]
    for d in range(RING):
        zs = lax.rem(meta[0] - d + RING, RING)
        dkv[zs] = got[d][pl.ds(PAIR, PAIR), :]
        for r in range(REPS):
            dq[:, pl.ds(d * QW + r * D, D)] = first[d, pl.ds(r * TOK, TOK), :]
            col = pl.multiple_of(zs * QW + (REPS + r) * D, D)
            dq[:, pl.ds(col, D)] = got[d][pl.ds(r * TOK, TOK), :]


def unpack_q(meta, first, got):
    return pl.pallas_call(
        unpack_q_body,
        out_shape=[
            jax.ShapeDtypeStruct((TOK, HQ * D), BF16),
            pltpu.VMEM((RING, PAIR, D), BF16),
        ],
        in_specs=[SM] + [VM] * (RING + 1),
        out_specs=[VM, VM],
        compiler_params=pltpu.CompilerParams(vmem_limit_bytes=12 * 2**20),
        name="unpackq",
    )(meta, keep(first), got[0], *[keep(m) for m in got[1:]])


def unpack_kv_body(a, b, dk, dv):
    for d in range(RING):
        for g, src in enumerate((a, b)):
            cols = pl.ds(d * KW + g * D, D)
            dk[:, cols] = src[d, pl.ds(0, TOK), :]
            dv[:, cols] = src[d, pl.ds(TOK, TOK), :]


def unpack_kv(a, b):
    return pl.pallas_call(
        unpack_kv_body,
        out_shape=[jax.ShapeDtypeStruct((TOK, KV * D), BF16)] * 2,
        in_specs=[VM, VM],
        out_specs=[VM, VM],
        compiler_params=pltpu.CompilerParams(vmem_limit_bytes=12 * 2**20),
        name="unpackkv",
    )(keep(a), keep(b))


def exchange(value):
    groups = lax.axis_size("head") // RING
    rows = [[g * RING + j for j in range(RING)] for g in range(groups)]
    return lax.all_to_all(value, "head", 0, 0, axis_index_groups=rows, tiled=True)


DISTANCES = (1, 7, 2, 6, 3, 5, 4)


def ring_send(parts):
    groups = lax.axis_size("head") // RING
    got = [parts[0]] + [None] * (RING - 1)
    for d in DISTANCES:
        pairs = [
            (g * RING + j, g * RING + (j + d) % RING) for g in range(groups) for j in range(RING)
        ]
        got[d] = lax.ppermute(parts[d], "head", pairs)
    return got


def group_shift(value, step):
    axes = ("seq", "head")
    count = lax.axis_size("seq") * lax.axis_size("head")
    shift = RING * step
    pairs = [(s, s + shift) for s in range(count) if 0 <= s + shift < count]
    return lax.ppermute(value, axes, pairs)


def shards(query, key_matrix, value_matrix, output_gradient, attn_out, doc_offsets, stats):
    member = lax.axis_index("head")
    z = member % RING
    base = (lax.axis_index("seq") * lax.axis_size("head") + member - z) * TOK
    meta_z = z[None].astype(jnp.int32)
    stats_t = stats.T.reshape(RING, HQ // RING, TOK)
    rows = (query, output_gradient, attn_out)
    parts = pack(0, (1, 7, 2, 6), meta_z, stats_t, *rows, key_matrix, value_matrix)
    keys0 = pack_keys(0, key_matrix, value_matrix)
    keys0 = exchange(keys0)
    parts |= pack(0, (3, 5, 4, 0), meta_z, stats_t, *rows, key_matrix, value_matrix)
    got0 = ring_send(parts)
    halo0 = group_shift(keys0, 1)
    parts = pack(1, tuple(range(RING)), meta_z, stats_t, *rows)
    got1 = ring_send(parts)
    keys1 = join(meta_z, got0)
    halo1 = group_shift(keys1, 1)
    position = base + jnp.arange(SPAN, dtype=jnp.int32)
    inner = doc_offsets[1:-1]
    start = jnp.max(jnp.where(inner[None, :] <= position[:, None], inner[None, :], 0), axis=1)
    starts = (start - base + SPAN).reshape(RING, TOK)
    meta = jnp.concatenate([meta_z, starts[:, 0] // PAIR])
    dq0, back0, own0 = attn(0, meta, starts, keys0, halo0, got0, keep)
    back0 = group_shift(back0, -1)
    dq0 = exchange(dq0)
    dq1, back1, own1 = attn(1, meta, starts, keys1, halo1, got1, keep)
    back1 = group_shift(back1, -1)
    parts = merge(meta_z, dq1, own0, back0)
    mixed = ring_send(parts)
    dkv1 = finish(own1, back1)
    dkv1 = exchange(dkv1)
    grad_query, dkv0 = unpack_q(meta_z, dq0, mixed)
    key_gradient, value_gradient = unpack_kv(dkv0, dkv1)
    return grad_query, key_gradient, value_gradient


def solution(mesh):
    placed = P(("seq", "head"), None)

    return jax.shard_map(
        shards,
        mesh=mesh,
        in_specs=(placed,) * 5 + (P(), placed),
        out_specs=(placed,) * 3,
        check_vma=False,
    )
```
